32 devices in a mesh: tm: 16 (over z, x, core), space: 2 (over y).
Axes of the slice: x: 2, y: 2, z: 4, core: 2. Of those that a mesh axis runs over, the one named last changes fastest.
Arguments:
- forcing: float32 [16, 8, 128, 128], P('tm', 'space'), may hold values from -6 to 6
- initial: float32 [8, 128, 128], P('space'), may hold values from -6 to 6
- coupling: float32 [8, 128, 128], P('space'), may hold values from 0.3 to 3
- velocity: float32 [3, 8, 128, 128], P(None, 'space'), may hold values from -0.9 to 0.9
Outputs:
- iterate: float32 [16, 8, 128, 128], P('tm', 'space')
The draws below stay inside these ranges and needn't reach their ends.
All inputs are finite; a program needn't handle non-finite values.
Results may differ from the reference program's by a relative error of at most 0.0003.
Values sent between devices are 32-bit elements; how exact they have to be, the bound alone decides.
A program may use at most 64 MiB of HBM per device.

```python
import math
import jax
import jax.numpy as jnp
from jax import lax

NY = 128
NX = 128
ITERS = 2
SWEEPS = 8
NT = 16
NZ = 8


def level_of(stream_key, shape, cuts, low, top_value):
    level = 1.0
    for axis_at, parts in cuts:
        draws = jax.random.uniform(jax.random.fold_in(jax.random.fold_in(stream_key, 6), axis_at), (parts,), jnp.float32, low / len(cuts), top_value / len(cuts))
        level = level * jnp.repeat(jnp.exp(draws), shape[axis_at] // parts).reshape((-1,) + (1,) * (len(shape) - 1 - axis_at))
    return level


def gaussian(key, dims, width, reach, shards=(), kind=jnp.bfloat16):
    array = width * jax.random.normal(key, dims, jnp.float32)
    if shards:
        array = array * level_of(key, dims, shards, -0.22, 0.18)
    return jnp.clip(array, -reach, reach).astype(kind)


def setup_inputs(seed: int = 0) -> dict:
    arg_keys = jax.random.split(jax.random.key(seed), 5)
    forcing = gaussian(arg_keys[0], (NT, NZ, NY, NX), 1.0, 6.0, ((0, 16), (1, 2)), jnp.float32)
    initial = gaussian(arg_keys[1], (NZ, NY, NX), 1.0, 6.0, ((0, 2),), jnp.float32)
    coupling = jnp.clip(jnp.exp(math.log(3.0) - 2.3025851 * jax.random.uniform(arg_keys[2], (NZ, NY, NX), jnp.float32) ** level_of(arg_keys[2], (NZ, NY, NX), ((0, 2),), -0.2, 0.2)), 0.3, 3.0)
    velocity = jnp.clip(jax.random.uniform(arg_keys[3], (3, NZ, NY, NX), jnp.float32, -0.9, 0.9) * level_of(arg_keys[3], (3, NZ, NY, NX), ((1, 2),), -0.4, 0.0), -0.9, 0.9)
    return dict(forcing=forcing, initial=initial, coupling=coupling, velocity=velocity)


wrap_alpha = 0.1


def padded(field):
    widths = [(0, 0)] * (field.ndim - 3) + [(1, 1)] * 3
    return jnp.pad(field, widths)


def coupled(extended, coupling, advect):
    total = (coupling - advect[0]) * extended[..., 2:, 1:-1, 1:-1] + (coupling + advect[0]) * extended[..., :-2, 1:-1, 1:-1]
    total = total + (coupling - advect[1]) * extended[..., 1:-1, 2:, 1:-1] + (coupling + advect[1]) * extended[..., 1:-1, :-2, 1:-1]
    total = total + (coupling - advect[2]) * extended[..., 1:-1, 1:-1, 2:] + (coupling + advect[2]) * extended[..., 1:-1, 1:-1, :-2]
    return total


def tables(total_steps):
    indices = jnp.arange(total_steps, dtype=jnp.int32)
    products = (indices[:, None] * indices[None, :]) % total_steps
    angles = products.astype(jnp.float32) * (2.0 * math.pi / total_steps)
    return jnp.cos(angles), jnp.sin(angles)


def matmul(table, columns):
    return jnp.dot(table, columns, preferred_element_type=jnp.float32, precision=lax.Precision.HIGHEST)


def reference(forcing, initial, coupling, velocity):
    total_steps = forcing.shape[0]
    shape = forcing.shape
    advect = coupling[None] * velocity
    cosine, sine_table = tables(total_steps)
    steps_float = jnp.arange(total_steps, dtype=jnp.float32)
    time_weight = jnp.exp(math.log(wrap_alpha) * steps_float / total_steps)[:, None, None, None]
    radius = math.exp(math.log(wrap_alpha) / total_steps)
    angles = steps_float * (2.0 * math.pi / total_steps)
    shift_re = radius * jnp.cos(angles)
    shift_im = radius * jnp.sin(angles)
    iterate = jnp.broadcast_to(initial, shape).astype(jnp.float32)

    def solve(pieces):
        source_re, source_im, freq_re, freq_im = pieces
        diag_re = 1.0 + 6.0 * coupling - freq_re
        diag_im = freq_im
        modulus = diag_re * diag_re + diag_im * diag_im
        value_re = (source_re * diag_re + source_im * diag_im) / modulus
        value_im = (source_im * diag_re - source_re * diag_im) / modulus
        for sweep in range(SWEEPS):
            sum_re = source_re + coupled(padded(value_re), coupling, advect)
            sum_im = source_im + coupled(padded(value_im), coupling, advect)
            value_re = (sum_re * diag_re + sum_im * diag_im) / modulus
            value_im = (sum_im * diag_re - sum_re * diag_im) / modulus
        return value_re, value_im

    for repeat in range(ITERS):
        previous = jnp.concatenate([initial[None], iterate[:-1]], axis=0)
        residual = forcing - ((1.0 + 6.0 * coupling) * iterate - coupled(padded(iterate), coupling, advect)) + previous
        columns = (residual * time_weight).reshape(total_steps, -1)
        spec_re = matmul(cosine, columns).reshape(shape)
        spec_im = (-matmul(sine_table, columns)).reshape(shape)
        value_re, value_im = lax.map(solve, (spec_re, spec_im, shift_re, shift_im))
        inverse_part = (matmul(cosine, value_re.reshape(total_steps, -1)) - matmul(sine_table, value_im.reshape(total_steps, -1))) / total_steps
        iterate = iterate + inverse_part.reshape(shape) / time_weight
    return iterate
```

```python
import math

import jax
import jax.numpy as jnp
import numpy as np
from jax import lax
from jax.experimental import pallas as pl
from jax.experimental.pallas import tpu as pltpu
from jax.sharding import PartitionSpec as P

ITERS = 2
SWEEPS = 8
HALO = 8

wrap_alpha = 0.1


def forward_table(steps):
    n = np.arange(steps)
    gamma = wrap_alpha ** (n / steps)
    table = np.zeros((steps // 2, 2, steps))
    for u in range(steps // 2):
        angle = 2.0 * np.pi * ((u * n) % steps) / steps
        if u == 0:
            table[u, 0] = gamma
            table[u, 1] = (1.0 - 2.0 * (n % 2)) * gamma
        else:
            table[u, 0] = np.cos(angle) * gamma
            table[u, 1] = -np.sin(angle) * gamma
    return table


def inverse_table(steps):
    n = np.arange(steps)
    table = np.zeros((steps // 2, 2, steps))
    for u in range(steps // 2):
        angle = 2.0 * np.pi * ((u * n) % steps) / steps
        if u == 0:
            table[u, 0] = 1.0 / steps
            table[u, 1] = (1.0 - 2.0 * (n % 2)) / steps
        else:
            table[u, 0] = 2.0 * np.cos(angle) / steps
            table[u, 1] = -2.0 * np.sin(angle) / steps
    return table


def by_index(index, values):
    picked = jnp.float32(values[0])
    for at in range(1, len(values)):
        picked = jnp.where(index == at, jnp.float32(values[at]), picked)
    return picked


def kernel(
    dims,
    f_ref,
    k_ref,
    out_ref,
    times,
    fields,
    edge,
    kbuf,
    coef,
    pq,
    src,
    wa,
    wb,
    whalo,
    part,
    gathered,
    reduced,
    last,
    back,
    states,
    s1,
    r1,
    s2,
    r2,
    sk,
    rk,
    se,
    re,
    sw,
    rw,
    ss,
    rs,
    sg,
    rg,
    s3,
    r3,
    s4,
    r4,
):
    T, S, NY, NX, zl = dims
    U = T // 2
    NZ = zl * S
    C = zl * NY // T
    bands = 2 * S
    R = NY // bands
    RH = R + 2 * HALO
    q = C // R
    per_plane = NY // C
    planes = NZ // U
    rho = wrap_alpha ** (1.0 / T)
    forward = forward_table(T)
    inverse = inverse_table(T)
    n = np.arange(T)
    gamma = wrap_alpha ** (n / T)

    t = lax.axis_index("tm")
    s = lax.axis_index("space")
    unit = t // 2
    core = t % 2
    band = s * 2 + core
    zi = t // per_plane
    row0 = pl.multiple_of((t % per_plane) * C, 8)

    def device(tt, ts):
        return {"tm": tt, "space": ts}

    def remote(source, target, ssem, rsem, tt, ts):
        return pltpu.make_async_remote_copy(
            src_ref=source,
            dst_ref=target,
            send_sem=ssem,
            recv_sem=rsem,
            device_id=device(tt, ts),
            device_id_type=pl.DeviceIdType.MESH,
        )

    sent = []

    def send(source, target, ssem, rsem, tt, ts, valid=None, maybe_self=True):
        copy = remote(source, target, ssem, rsem, tt, ts)
        same = jnp.logical_and(tt == t, ts == s) if maybe_self else None
        away = valid
        if maybe_self:
            here = same if valid is None else jnp.logical_and(valid, same)
            away = jnp.logical_not(same)
            if valid is not None:
                away = jnp.logical_and(valid, away)

            @pl.when(here)
            def _():
                pltpu.make_async_copy(source, target, rsem).start()

        if away is None:
            copy.start()
            sent.append(copy.wait_send)
        else:

            @pl.when(away)
            def _():
                copy.start()

            def finish():
                @pl.when(away)
                def _():
                    copy.wait_send()

            sent.append(finish)

    def arrived(target, rsem, valid=None):
        if valid is None:
            pltpu.make_async_copy(target, target, rsem).wait()
        else:

            @pl.when(valid)
            def _():
                pltpu.make_async_copy(target, target, rsem).wait()

    for d in range(1, T):
        tt = lax.rem(t + d, T)
        send(
            f_ref.at[pl.ds(pl.multiple_of(tt * C, 8), C)],
            times.at[t],
            s1.at[d],
            r1.at[d],
            tt,
            s,
            maybe_self=False,
        )
    send(
        k_ref.at[4, zl - 1, pl.ds(row0 + HALO, C)],
        edge.at[0],
        se.at[0],
        re.at[0],
        t,
        jnp.minimum(s + 1, S - 1),
        valid=s + 1 < S,
        maybe_self=False,
    )
    send(
        k_ref.at[4, 0, pl.ds(row0 + HALO, C)],
        edge.at[1],
        se.at[1],
        re.at[1],
        t,
        jnp.maximum(s - 1, 0),
        valid=s > 0,
        maybe_self=False,
    )
    for d in range(S):
        ts = lax.rem(s + d, S)
        rows = pl.ds(pl.multiple_of((ts * 2 + core) * R, 8), RH)
        source = k_ref.at[pl.ds(0, 4), :, rows]
        target = kbuf.at[:, pl.ds(s * zl, zl)]
        if d:
            send(source, target, sk.at[d], rk.at[d], t, ts, maybe_self=False)
        else:
            pltpu.make_async_copy(source, target, rk.at[0]).start()
    times[pl.ds(t, 1)] = f_ref[pl.ds(pl.multiple_of(t * C, 8), C)][None]

    def shifted(value, by, axis):
        return pltpu.roll(value, by % value.shape[axis], axis)

    window = pl.ds(row0, C + 2 * HALO)
    inner = pl.ds(row0 + HALO, C)
    column = lax.broadcasted_iota(jnp.int32, (C, NX), 1)
    arrived(edge.at[0], re.at[0], valid=s > 0)
    arrived(edge.at[1], re.at[1], valid=s + 1 < S)

    @pl.when(s == 0)
    def _():
        edge[0] = jnp.zeros((C, NX), jnp.float32)

    @pl.when(s + 1 == S)
    def _():
        edge[1] = jnp.zeros((C, NX), jnp.float32)

    wide = k_ref[4, zi, window]
    middle = wide[HALO : HALO + C]
    lower = jnp.where(zi == 0, edge[0], k_ref[4, jnp.maximum(zi - 1, 0), inner])
    upper = jnp.where(zi == zl - 1, edge[1], k_ref[4, jnp.minimum(zi + 1, zl - 1), inner])
    coupling = k_ref[0, zi, inner]
    adz = coupling * k_ref[1, zi, inner]
    ady = coupling * k_ref[2, zi, inner]
    adx = coupling * k_ref[3, zi, inner]
    summed = (coupling - adz) * upper + (coupling + adz) * lower
    summed += (coupling - ady) * shifted(wide, -1, 0)[HALO : HALO + C]
    summed += (coupling + ady) * shifted(wide, 1, 0)[HALO : HALO + C]
    summed += (coupling - adx) * jnp.where(column == NX - 1, 0.0, shifted(middle, -1, 1))
    summed += (coupling + adx) * jnp.where(column == 0, 0.0, shifted(middle, 1, 1))
    start = summed - 6.0 * coupling * middle

    for d in range(1, T):
        arrived(times.at[lax.rem(t + T - d, T)], r1.at[d])

    for block in range(C // 8):
        rows = slice(block * 8, block * 8 + 8)
        values = [times[m, rows] + start[rows] for m in range(T)]
        for u in range(U):
            for p in range(2):
                total = values[0] * float(forward[u, p, 0])
                for m in range(1, T):
                    total = total + values[m] * float(forward[u, p, m])
                fields[u, p, rows] = total

    z = s * zl + zi
    for step in range(U):
        u = lax.rem(unit + step, U)
        for o in range(q):
            b = (t % per_plane) * q + o
            for kind in range(3):
                to = b + (0, -1, 1)[kind]
                valid = (None, to >= 0, to < bands)[kind]
                safe = jnp.clip(to, 0, bands - 1)
                first, count, land = (
                    (o * R, R, HALO),
                    (o * R, HALO, HALO + R),
                    (o * R + R - HALO, HALO, 0),
                )[kind]
                send(
                    fields.at[u, :, pl.ds(first, count)],
                    src.at[:, z, pl.ds(land, count)],
                    s2.at[step, o, kind],
                    r2.at[z, kind],
                    u * 2 + safe % 2,
                    safe // 2,
                    valid=valid,
                )

    for d in range(S):
        arrived(kbuf.at[:, pl.ds(lax.rem(s + S - d, S) * zl, zl)], rk.at[d])
    angles = [2.0 * math.pi * u / U / 2 for u in range(U)]
    shift_re1 = by_index(unit, [rho * math.cos(a) for a in angles])
    shift_im1 = by_index(unit, [0.0] + [rho * math.sin(a) for a in angles[1:]])
    shift_re2 = by_index(unit, [-rho] + [rho * math.cos(a) for a in angles[1:]])
    wide_column = lax.broadcasted_iota(jnp.int32, (RH, NX), 1)

    @pl.loop(0, NZ)
    def _(z):
        c = kbuf[0, z]
        az = c * kbuf[1, z]
        ay = c * kbuf[2, z]
        ax = c * kbuf[3, z]
        zero = jnp.zeros_like(c)
        coef[0, z] = jnp.where(z == NZ - 1, zero, c - az)
        coef[1, z] = jnp.where(z == 0, zero, c + az)
        coef[2, z] = c - ay
        coef[3, z] = c + ay
        coef[4, z] = jnp.where(wide_column == NX - 1, zero, c - ax)
        coef[5, z] = jnp.where(wide_column == 0, zero, c + ax)
        diag1 = 1.0 + 6.0 * c - shift_re1
        diag2 = 1.0 + 6.0 * c - shift_re2
        im2 = shift_im1 * shift_im1
        modulus1 = diag1 * diag1 + im2
        modulus2 = diag2 * diag2 + im2
        pq[0, z] = diag1 / modulus1
        pq[1, z] = diag2 / modulus2
        pq[2, z] = shift_im1 / modulus1

    @pl.when(band == 0)
    def _():
        src[:, :, :HALO] = jnp.zeros((2, NZ, HALO, NX), jnp.float32)
        last[:, :HALO] = jnp.zeros((NZ, HALO, NX), jnp.float32)
        whalo[0] = jnp.zeros((2, NZ, HALO, NX), jnp.float32)

    @pl.when(band == bands - 1)
    def _():
        src[:, :, HALO + R :] = jnp.zeros((2, NZ, HALO, NX), jnp.float32)
        last[:, HALO + R :] = jnp.zeros((NZ, HALO, NX), jnp.float32)
        whalo[1] = jnp.zeros((2, NZ, HALO, NX), jnp.float32)

    for z in range(NZ):
        arrived(src.at[:, z, pl.ds(HALO, R)], r2.at[z, 0])
        arrived(src.at[:, z, pl.ds(HALO + R, HALO)], r2.at[z, 1], valid=band < bands - 1)
        arrived(src.at[:, z, pl.ds(0, HALO)], r2.at[z, 2], valid=band > 0)

    def scale(z, re_part, im_part, target):
        p1, p2, im = pq[0, z], pq[1, z], pq[2, z]
        target[0, z] = re_part * p1 + im_part * im
        target[1, z] = im_part * p2 - re_part * im

    def sweep(old, new):
        @pl.loop(0, NZ)
        def _(z):
            up = jnp.minimum(z + 1, NZ - 1)
            down = jnp.maximum(z - 1, 0)
            sums = []
            for p in range(2):
                here = old[p, z]
                total = src[p, z] + coef[0, z] * old[p, up] + coef[1, z] * old[p, down]
                total += coef[2, z] * shifted(here, -1, 0) + coef[3, z] * shifted(here, 1, 0)
                total += coef[4, z] * shifted(here, -1, 1) + coef[5, z] * shifted(here, 1, 1)
                sums.append(total)
            scale(z, sums[0], sums[1], new)

    @pl.loop(0, NZ)
    def _(z):
        scale(z, src[0, z], src[1, z], wa)

    @pl.loop(0, SWEEPS // 2)
    def _(i):
        sweep(wa, wb)
        sweep(wb, wa)

    below = jnp.maximum(band - 1, 0)
    above = jnp.minimum(band + 1, bands - 1)
    send(
        wa.at[:, :, pl.ds(HALO + R - HALO, HALO)],
        whalo.at[0],
        sw.at[0],
        rw.at[0],
        unit * 2 + above % 2,
        above // 2,
        valid=band < bands - 1,
        maybe_self=False,
    )
    send(
        wa.at[:, :, pl.ds(HALO, HALO)],
        whalo.at[1],
        sw.at[1],
        rw.at[1],
        unit * 2 + below % 2,
        below // 2,
        valid=band > 0,
        maybe_self=False,
    )
    weight_re = by_index(unit, [float(inverse[u, 0, T - 1]) for u in range(U)])
    weight_im = by_index(unit, [float(inverse[u, 1, T - 1]) for u in range(U)])

    @pl.loop(0, NZ)
    def _(z):
        part[z] = weight_re * wa[0, z, HALO : HALO + R] + weight_im * wa[1, z, HALO : HALO + R]

    for d in range(1, U):
        u = lax.rem(unit + d, U)
        send(
            part.at[pl.ds(u * planes, planes)],
            gathered.at[unit],
            ss.at[d],
            rs.at[d],
            u * 2 + core,
            s,
            maybe_self=False,
        )
    gathered[pl.ds(unit, 1)] = part[pl.ds(unit * planes, planes)][None]
    for d in range(1, U):
        arrived(gathered.at[lax.rem(unit + U - d, U)], rs.at[d])
    total = gathered[0]
    for u in range(1, U):
        total = total + gathered[u]
    reduced[...] = total * rho
    mine = pl.ds(unit * planes, planes)
    for d in range(U):
        u = lax.rem(unit + d, U)
        for kind in range(3):
            to = band + (0, -1, 1)[kind]
            valid = (None, to >= 0, to < bands)[kind]
            safe = jnp.clip(to, 0, bands - 1)
            first, count, land = ((0, R, HALO), (0, HALO, HALO + R), (R - HALO, HALO, 0))[kind]
            if kind == 0 and d == 0:
                last[mine, HALO : HALO + R] = reduced[...]
                continue
            send(
                reduced.at[:, pl.ds(first, count)],
                last.at[mine, pl.ds(land, count)],
                sg.at[d, kind],
                rg.at[d, kind],
                u * 2 + safe % 2,
                safe // 2,
                valid=valid,
                maybe_self=False,
            )
    arrived(whalo.at[0], rw.at[0], valid=band > 0)
    arrived(whalo.at[1], rw.at[1], valid=band < bands - 1)
    sent_before = list(sent)
    sent.clear()
    for finish in sent_before:
        finish()
    wa[:, :, :HALO] = whalo[0]
    wa[:, :, HALO + R :] = whalo[1]
    for d in range(U):
        theirs = pl.ds(lax.rem(unit + U - d, U) * planes, planes)
        if d:
            arrived(last.at[theirs, pl.ds(HALO, R)], rg.at[d, 0])
        arrived(last.at[theirs, pl.ds(HALO + R, HALO)], rg.at[d, 1], valid=band < bands - 1)
        arrived(last.at[theirs, pl.ds(0, HALO)], rg.at[d, 2], valid=band > 0)

    @pl.loop(0, NZ)
    def _(z):
        src[0, z] = src[0, z] - last[z]
        src[1, z] = src[1, z] - jnp.where(unit == 0, last[z], jnp.zeros_like(last[z]))

    @pl.loop(0, SWEEPS // 2)
    def _(i):
        sweep(wa, wb)
        sweep(wb, wa)

    sweep(wa, wb)

    for step in range(NZ):
        z = lax.rem(unit * planes + step, NZ)
        at = (z % zl) * per_plane + (band * R) // C
        offset = pl.multiple_of((band * R) % C, 8)
        send(
            wb.at[:, z, pl.ds(HALO, R)],
            back.at[unit, :, pl.ds(offset, R)],
            s3.at[step],
            r3.at[unit, lax.rem(band, q)],
            at,
            z // zl,
        )
    for u in range(U):
        for o in range(q):
            arrived(back.at[u, :, pl.ds(o * R, R)], r3.at[u, o])
    for block in range(C // 8):
        rows = slice(block * 8, block * 8 + 8)
        values = [back[u, p, rows] for u in range(U) for p in range(2)]
        begin = middle[rows]
        for m in range(T):
            total = begin
            for at in range(T):
                total = total + values[at] * float(inverse[at // 2, at % 2, m] / gamma[m])
            states[m, rows] = total
    for d in range(1, T):
        tt = lax.rem(t + d, T)
        send(
            states.at[tt],
            out_ref.at[pl.ds(pl.multiple_of(t * C, 8), C)],
            s4.at[d],
            r4.at[d],
            tt,
            s,
            maybe_self=False,
        )
    out_ref[pl.ds(pl.multiple_of(t * C, 8), C)] = states[pl.ds(t, 1)][0]
    for d in range(1, T):
        tt = lax.rem(t + T - d, T)
        arrived(out_ref.at[pl.ds(pl.multiple_of(tt * C, 8), C)], r4.at[d])
    for finish in sent:
        finish()


def body(forcing, initial, coupling, velocity):
    local_steps, zl, NY, NX = forcing.shape
    T = lax.axis_size("tm")
    S = lax.axis_size("space")
    U = T // 2
    NZ = zl * S
    C = zl * NY // T
    bands = 2 * S
    R = NY // bands
    RH = R + 2 * HALO
    q = C // R
    planes = NZ // U
    assert local_steps == 1 and SWEEPS <= HALO <= R and ITERS == 2
    assert C % R == 0 and NY % C == 0 and NZ % U == 0
    stacked = jnp.concatenate([coupling[None], velocity, initial[None]], axis=0)
    stacked = jnp.pad(stacked, ((0, 0), (0, 0), (HALO, HALO), (0, 0)))
    f32 = jnp.float32
    dma = pltpu.SemaphoreType.DMA
    out = pl.pallas_call(
        lambda *refs: kernel((T, S, NY, NX, zl), *refs),
        out_shape=jax.ShapeDtypeStruct((zl * NY, NX), f32),
        in_specs=[pl.BlockSpec(memory_space=pltpu.VMEM)] * 2,
        out_specs=pl.BlockSpec(memory_space=pltpu.VMEM),
        scratch_shapes=[
            pltpu.VMEM((T, C, NX), f32),
            pltpu.VMEM((U, 2, C, NX), f32),
            pltpu.VMEM((2, C, NX), f32),
            pltpu.VMEM((4, NZ, RH, NX), f32),
            pltpu.VMEM((6, NZ, RH, NX), f32),
            pltpu.VMEM((3, NZ, RH, NX), f32),
            pltpu.VMEM((2, NZ, RH, NX), f32),
            pltpu.VMEM((2, NZ, RH, NX), f32),
            pltpu.VMEM((2, NZ, RH, NX), f32),
            pltpu.VMEM((2, 2, NZ, HALO, NX), f32),
            pltpu.VMEM((NZ, R, NX), f32),
            pltpu.VMEM((U, planes, R, NX), f32),
            pltpu.VMEM((planes, R, NX), f32),
            pltpu.VMEM((NZ, RH, NX), f32),
            pltpu.VMEM((U, 2, C, NX), f32),
            pltpu.VMEM((T, C, NX), f32),
            dma((T,)),
            dma((T,)),
            dma((U, q, 3)),
            dma((NZ, 3)),
            dma((S,)),
            dma((S,)),
            dma((2,)),
            dma((2,)),
            dma((2,)),
            dma((2,)),
            dma((U,)),
            dma((U,)),
            dma((U, 3)),
            dma((U, 3)),
            dma((NZ,)),
            dma((U, q)),
            dma((T,)),
            dma((T,)),
        ],
        compiler_params=pltpu.CompilerParams(
            has_side_effects=True, vmem_limit_bytes=48 * 1024 * 1024
        ),
    )(forcing.reshape(zl * NY, NX), stacked)
    return out.reshape(forcing.shape)


def solution(mesh):
    return jax.shard_map(
        body,
        mesh=mesh,
        in_specs=(
            P("tm", "space", None, None),
            P("space", None, None),
            P("space", None, None),
            P(None, "space", None, None),
        ),
        out_specs=P("tm", "space", None, None),
        check_vma=False,
    )
```

```python
import math

import jax
import jax.numpy as jnp
import numpy as np
from jax import lax
from jax.experimental import pallas as pl
from jax.experimental.pallas import tpu as pltpu
from jax.sharding import PartitionSpec as P

ITERS = 2
SWEEPS = 8
HALO = 8

wrap_alpha = 0.1


def forward_table(steps):
    n = np.arange(steps)
    gamma = wrap_alpha ** (n / steps)
    table = np.zeros((steps // 2, 2, steps))
    for u in range(steps // 2):
        angle = 2.0 * np.pi * ((u * n) % steps) / steps
        if u == 0:
            table[u, 0] = gamma
            table[u, 1] = (1.0 - 2.0 * (n % 2)) * gamma
        else:
            table[u, 0] = np.cos(angle) * gamma
            table[u, 1] = -np.sin(angle) * gamma
    return table


def inverse_table(steps):
    n = np.arange(steps)
    table = np.zeros((steps // 2, 2, steps))
    for u in range(steps // 2):
        angle = 2.0 * np.pi * ((u * n) % steps) / steps
        if u == 0:
            table[u, 0] = 1.0 / steps
            table[u, 1] = (1.0 - 2.0 * (n % 2)) / steps
        else:
            table[u, 0] = 2.0 * np.cos(angle) / steps
            table[u, 1] = -2.0 * np.sin(angle) / steps
    return table


def by_index(index, values):
    picked = jnp.float32(values[0])
    for at in range(1, len(values)):
        picked = jnp.where(index == at, jnp.float32(values[at]), picked)
    return picked


def kernel(
    dims,
    f_ref,
    k_ref,
    out_ref,
    times,
    fields,
    edge,
    kbuf,
    coef,
    pq,
    src,
    wa,
    wb,
    whalo,
    part,
    gathered,
    reduced,
    last,
    back,
    states,
    s1,
    r1,
    s2,
    r2,
    sk,
    rk,
    se,
    re,
    sw,
    rw,
    ss,
    rs,
    sg,
    rg,
    s3,
    r3,
    s4,
    r4,
):
    T, S, NY, NX, zl = dims
    U = T // 2
    NZ = zl * S
    C = zl * NY // T
    bands = 2 * S
    R = NY // bands
    RH = R + 2 * HALO
    q = C // R
    planes = NZ // U
    rho = wrap_alpha ** (1.0 / T)
    forward = forward_table(T)
    inverse = inverse_table(T)
    n = np.arange(T)
    gamma = wrap_alpha ** (n / T)

    t = lax.axis_index("tm")
    s = lax.axis_index("space")
    group = t // zl
    zi = t % zl
    unit = (zi * S + s) // q
    band = group * q + (zi * S + s) % q
    row0 = pl.multiple_of(group * C, 8)

    def place(u, b):
        at = u * q + b % q
        return (b // q) * zl + at // S, at % S

    def chunk(tt):
        start = (tt % zl) * NY + (tt // zl) * C
        return pl.ds(pl.multiple_of(start, 8), C)

    far_first = sorted(range(1, T), key=lambda d: -min(d, T - d))

    def device(tt, ts):
        return {"tm": tt, "space": ts}

    def remote(source, target, ssem, rsem, tt, ts):
        return pltpu.make_async_remote_copy(
            src_ref=source,
            dst_ref=target,
            send_sem=ssem,
            recv_sem=rsem,
            device_id=device(tt, ts),
            device_id_type=pl.DeviceIdType.MESH,
        )

    sent = []

    def send(source, target, ssem, rsem, tt, ts, valid=None, maybe_self=True):
        copy = remote(source, target, ssem, rsem, tt, ts)
        same = jnp.logical_and(tt == t, ts == s) if maybe_self else None
        away = valid
        if maybe_self:
            here = same if valid is None else jnp.logical_and(valid, same)
            away = jnp.logical_not(same)
            if valid is not None:
                away = jnp.logical_and(valid, away)

            @pl.when(here)
            def _():
                pltpu.make_async_copy(source, target, rsem).start()

        if away is None:
            copy.start()
            sent.append(copy.wait_send)
        else:

            @pl.when(away)
            def _():
                copy.start()

            def finish():
                @pl.when(away)
                def _():
                    copy.wait_send()

            sent.append(finish)

    def arrived(target, rsem, valid=None):
        if valid is None:
            pltpu.make_async_copy(target, target, rsem).wait()
        else:

            @pl.when(valid)
            def _():
                pltpu.make_async_copy(target, target, rsem).wait()

    for d in far_first:
        tt = lax.rem(t + d, T)
        send(
            f_ref.at[chunk(tt)],
            times.at[t],
            s1.at[d],
            r1.at[d],
            tt,
            s,
            maybe_self=False,
        )
    send(
        k_ref.at[4, zl - 1, pl.ds(row0 + HALO, C)],
        edge.at[0],
        se.at[0],
        re.at[0],
        t,
        jnp.minimum(s + 1, S - 1),
        valid=s + 1 < S,
        maybe_self=False,
    )
    send(
        k_ref.at[4, 0, pl.ds(row0 + HALO, C)],
        edge.at[1],
        se.at[1],
        re.at[1],
        t,
        jnp.maximum(s - 1, 0),
        valid=s > 0,
        maybe_self=False,
    )
    for d in range(S):
        ts = lax.rem(s + d, S)
        rows = pl.ds(pl.multiple_of((group * q + (zi * S + ts) % q) * R, 8), RH)
        source = k_ref.at[pl.ds(0, 4), :, rows]
        target = kbuf.at[:, pl.ds(s * zl, zl)]
        if d:
            send(source, target, sk.at[d], rk.at[d], t, ts, maybe_self=False)
        else:
            pltpu.make_async_copy(source, target, rk.at[0]).start()
    times[pl.ds(t, 1)] = f_ref[chunk(t)][None]

    def shifted(value, by, axis):
        return pltpu.roll(value, by % value.shape[axis], axis)

    window = pl.ds(row0, C + 2 * HALO)
    inner = pl.ds(row0 + HALO, C)
    column = lax.broadcasted_iota(jnp.int32, (C, NX), 1)
    arrived(edge.at[0], re.at[0], valid=s > 0)
    arrived(edge.at[1], re.at[1], valid=s + 1 < S)

    @pl.when(s == 0)
    def _():
        edge[0] = jnp.zeros((C, NX), jnp.float32)

    @pl.when(s + 1 == S)
    def _():
        edge[1] = jnp.zeros((C, NX), jnp.float32)

    wide = k_ref[4, zi, window]
    middle = wide[HALO : HALO + C]
    lower = jnp.where(zi == 0, edge[0], k_ref[4, jnp.maximum(zi - 1, 0), inner])
    upper = jnp.where(zi == zl - 1, edge[1], k_ref[4, jnp.minimum(zi + 1, zl - 1), inner])
    coupling = k_ref[0, zi, inner]
    adz = coupling * k_ref[1, zi, inner]
    ady = coupling * k_ref[2, zi, inner]
    adx = coupling * k_ref[3, zi, inner]
    summed = (coupling - adz) * upper + (coupling + adz) * lower
    summed += (coupling - ady) * shifted(wide, -1, 0)[HALO : HALO + C]
    summed += (coupling + ady) * shifted(wide, 1, 0)[HALO : HALO + C]
    summed += (coupling - adx) * jnp.where(column == NX - 1, 0.0, shifted(middle, -1, 1))
    summed += (coupling + adx) * jnp.where(column == 0, 0.0, shifted(middle, 1, 1))
    start = summed - 6.0 * coupling * middle

    for d in range(1, T):
        arrived(times.at[lax.rem(t + T - d, T)], r1.at[d])

    for block in range(C // 8):
        rows = slice(block * 8, block * 8 + 8)
        values = [times[m, rows] + start[rows] for m in range(T)]
        for u in range(U):
            for p in range(2):
                total = values[0] * float(forward[u, p, 0])
                for m in range(1, T):
                    total = total + values[m] * float(forward[u, p, m])
                fields[u, p, rows] = total

    z = s * zl + zi
    for step in range(U):
        u = lax.rem(unit + step, U)
        for o in range(q):
            b = group * q + o
            for kind in range(3):
                to = b + (0, -1, 1)[kind]
                valid = (None, to >= 0, to < bands)[kind]
                safe = jnp.clip(to, 0, bands - 1)
                first, count, land = (
                    (o * R, R, HALO),
                    (o * R, HALO, HALO + R),
                    (o * R + R - HALO, HALO, 0),
                )[kind]
                to_t, to_s = place(u, safe)
                send(
                    fields.at[u, :, pl.ds(first, count)],
                    src.at[:, z, pl.ds(land, count)],
                    s2.at[step, o, kind],
                    r2.at[z, kind],
                    to_t,
                    to_s,
                    valid=valid,
                )

    for d in range(S):
        arrived(kbuf.at[:, pl.ds(lax.rem(s + S - d, S) * zl, zl)], rk.at[d])
    angles = [2.0 * math.pi * u / U / 2 for u in range(U)]
    shift_re1 = by_index(unit, [rho * math.cos(a) for a in angles])
    shift_im1 = by_index(unit, [0.0] + [rho * math.sin(a) for a in angles[1:]])
    shift_re2 = by_index(unit, [-rho] + [rho * math.cos(a) for a in angles[1:]])
    wide_column = lax.broadcasted_iota(jnp.int32, (RH, NX), 1)

    @pl.loop(0, NZ)
    def _(z):
        c = kbuf[0, z]
        az = c * kbuf[1, z]
        ay = c * kbuf[2, z]
        ax = c * kbuf[3, z]
        zero = jnp.zeros_like(c)
        coef[0, z] = jnp.where(z == NZ - 1, zero, c - az)
        coef[1, z] = jnp.where(z == 0, zero, c + az)
        coef[2, z] = c - ay
        coef[3, z] = c + ay
        coef[4, z] = jnp.where(wide_column == NX - 1, zero, c - ax)
        coef[5, z] = jnp.where(wide_column == 0, zero, c + ax)
        diag1 = 1.0 + 6.0 * c - shift_re1
        diag2 = 1.0 + 6.0 * c - shift_re2
        im2 = shift_im1 * shift_im1
        modulus1 = diag1 * diag1 + im2
        modulus2 = diag2 * diag2 + im2
        pq[0, z] = diag1 / modulus1
        pq[1, z] = diag2 / modulus2
        pq[2, z] = shift_im1 / modulus1

    @pl.when(band == 0)
    def _():
        src[:, :, :HALO] = jnp.zeros((2, NZ, HALO, NX), jnp.float32)
        last[:, :HALO] = jnp.zeros((NZ, HALO, NX), jnp.float32)
        whalo[0] = jnp.zeros((2, NZ, HALO, NX), jnp.float32)

    @pl.when(band == bands - 1)
    def _():
        src[:, :, HALO + R :] = jnp.zeros((2, NZ, HALO, NX), jnp.float32)
        last[:, HALO + R :] = jnp.zeros((NZ, HALO, NX), jnp.float32)
        whalo[1] = jnp.zeros((2, NZ, HALO, NX), jnp.float32)

    for z in range(NZ):
        arrived(src.at[:, z, pl.ds(HALO, R)], r2.at[z, 0])
        arrived(src.at[:, z, pl.ds(HALO + R, HALO)], r2.at[z, 1], valid=band < bands - 1)
        arrived(src.at[:, z, pl.ds(0, HALO)], r2.at[z, 2], valid=band > 0)

    def scale(z, re_part, im_part, target):
        p1, p2, im = pq[0, z], pq[1, z], pq[2, z]
        target[0, z] = re_part * p1 + im_part * im
        target[1, z] = im_part * p2 - re_part * im

    together = math.gcd(NZ, 8)

    def sweep(old, new):
        @pl.loop(0, NZ // together)
        def _(trip):
            for o in range(together):
                z = trip * together + o
                up = jnp.minimum(z + 1, NZ - 1) if o == together - 1 else z + 1
                down = jnp.maximum(z - 1, 0) if o == 0 else z - 1
                sums = []
                for p in range(2):
                    here = old[p, z]
                    total = src[p, z] + coef[0, z] * old[p, up] + coef[1, z] * old[p, down]
                    total += coef[2, z] * shifted(here, -1, 0) + coef[3, z] * shifted(here, 1, 0)
                    total += coef[4, z] * shifted(here, -1, 1) + coef[5, z] * shifted(here, 1, 1)
                    sums.append(total)
                scale(z, sums[0], sums[1], new)

    @pl.loop(0, NZ)
    def _(z):
        scale(z, src[0, z], src[1, z], wa)

    @pl.loop(0, SWEEPS // 2)
    def _(i):
        sweep(wa, wb)
        sweep(wb, wa)

    below = jnp.maximum(band - 1, 0)
    above = jnp.minimum(band + 1, bands - 1)
    send(
        wa.at[:, :, pl.ds(HALO + R - HALO, HALO)],
        whalo.at[0],
        sw.at[0],
        rw.at[0],
        *place(unit, above),
        valid=band < bands - 1,
        maybe_self=False,
    )
    send(
        wa.at[:, :, pl.ds(HALO, HALO)],
        whalo.at[1],
        sw.at[1],
        rw.at[1],
        *place(unit, below),
        valid=band > 0,
        maybe_self=False,
    )
    weight_re = by_index(unit, [float(inverse[u, 0, T - 1]) for u in range(U)])
    weight_im = by_index(unit, [float(inverse[u, 1, T - 1]) for u in range(U)])

    @pl.loop(0, NZ)
    def _(z):
        part[z] = weight_re * wa[0, z, HALO : HALO + R] + weight_im * wa[1, z, HALO : HALO + R]

    for d in range(1, U):
        u = lax.rem(unit + d, U)
        send(
            part.at[pl.ds(u * planes, planes)],
            gathered.at[unit],
            ss.at[d],
            rs.at[d],
            *place(u, band),
            maybe_self=False,
        )
    gathered[pl.ds(unit, 1)] = part[pl.ds(unit * planes, planes)][None]
    for d in range(1, U):
        arrived(gathered.at[lax.rem(unit + U - d, U)], rs.at[d])
    total = gathered[0]
    for u in range(1, U):
        total = total + gathered[u]
    reduced[...] = total * rho
    mine = pl.ds(unit * planes, planes)
    for d in range(U):
        u = lax.rem(unit + d, U)
        for kind in range(3):
            to = band + (0, -1, 1)[kind]
            valid = (None, to >= 0, to < bands)[kind]
            safe = jnp.clip(to, 0, bands - 1)
            first, count, land = ((0, R, HALO), (0, HALO, HALO + R), (R - HALO, HALO, 0))[kind]
            if kind == 0 and d == 0:
                last[mine, HALO : HALO + R] = reduced[...]
                continue
            send(
                reduced.at[:, pl.ds(first, count)],
                last.at[mine, pl.ds(land, count)],
                sg.at[d, kind],
                rg.at[d, kind],
                *place(u, safe),
                valid=valid,
                maybe_self=False,
            )
    arrived(whalo.at[0], rw.at[0], valid=band > 0)
    arrived(whalo.at[1], rw.at[1], valid=band < bands - 1)
    sent_before = list(sent)
    sent.clear()
    for finish in sent_before:
        finish()
    wa[:, :, :HALO] = whalo[0]
    wa[:, :, HALO + R :] = whalo[1]
    for d in range(U):
        theirs = pl.ds(lax.rem(unit + U - d, U) * planes, planes)
        if d:
            arrived(last.at[theirs, pl.ds(HALO, R)], rg.at[d, 0])
        arrived(last.at[theirs, pl.ds(HALO + R, HALO)], rg.at[d, 1], valid=band < bands - 1)
        arrived(last.at[theirs, pl.ds(0, HALO)], rg.at[d, 2], valid=band > 0)

    @pl.loop(0, NZ)
    def _(z):
        src[0, z] = src[0, z] - last[z]
        src[1, z] = src[1, z] - jnp.where(unit == 0, last[z], jnp.zeros_like(last[z]))

    @pl.loop(0, SWEEPS // 2)
    def _(i):
        sweep(wa, wb)
        sweep(wb, wa)

    sweep(wa, wb)

    for step in range(NZ):
        z = lax.rem(unit * planes + step, NZ)
        at = group * zl + z % zl
        offset = pl.multiple_of((band % q) * R, 8)
        send(
            wb.at[:, z, pl.ds(HALO, R)],
            back.at[unit, :, pl.ds(offset, R)],
            s3.at[step],
            r3.at[unit, lax.rem(band, q)],
            at,
            z // zl,
        )
    for u in range(U):
        for o in range(q):
            arrived(back.at[u, :, pl.ds(o * R, R)], r3.at[u, o])
    for block in range(C // 8):
        rows = slice(block * 8, block * 8 + 8)
        values = [back[u, p, rows] for u in range(U) for p in range(2)]
        begin = middle[rows]
        for m in range(T):
            total = begin
            for at in range(T):
                total = total + values[at] * float(inverse[at // 2, at % 2, m] / gamma[m])
            states[m, rows] = total
    for d in far_first:
        tt = lax.rem(t + d, T)
        send(
            states.at[tt],
            out_ref.at[chunk(t)],
            s4.at[d],
            r4.at[d],
            tt,
            s,
            maybe_self=False,
        )
    out_ref[chunk(t)] = states[pl.ds(t, 1)][0]
    for d in range(1, T):
        tt = lax.rem(t + T - d, T)
        arrived(out_ref.at[chunk(tt)], r4.at[d])
    for finish in sent:
        finish()


def body(forcing, initial, coupling, velocity):
    local_steps, zl, NY, NX = forcing.shape
    T = lax.axis_size("tm")
    S = lax.axis_size("space")
    U = T // 2
    NZ = zl * S
    C = zl * NY // T
    bands = 2 * S
    R = NY // bands
    RH = R + 2 * HALO
    q = C // R
    planes = NZ // U
    assert local_steps == 1 and SWEEPS <= HALO <= R and ITERS == 2
    assert C % R == 0 and NY % C == 0 and NZ % U == 0
    stacked = jnp.concatenate([coupling[None], velocity, initial[None]], axis=0)
    stacked = jnp.pad(stacked, ((0, 0), (0, 0), (HALO, HALO), (0, 0)))
    f32 = jnp.float32
    dma = pltpu.SemaphoreType.DMA
    out = pl.pallas_call(
        lambda *refs: kernel((T, S, NY, NX, zl), *refs),
        out_shape=jax.ShapeDtypeStruct((zl * NY, NX), f32),
        in_specs=[pl.BlockSpec(memory_space=pltpu.VMEM)] * 2,
        out_specs=pl.BlockSpec(memory_space=pltpu.VMEM),
        scratch_shapes=[
            pltpu.VMEM((T, C, NX), f32),
            pltpu.VMEM((U, 2, C, NX), f32),
            pltpu.VMEM((2, C, NX), f32),
            pltpu.VMEM((4, NZ, RH, NX), f32),
            pltpu.VMEM((6, NZ, RH, NX), f32),
            pltpu.VMEM((3, NZ, RH, NX), f32),
            pltpu.VMEM((2, NZ, RH, NX), f32),
            pltpu.VMEM((2, NZ, RH, NX), f32),
            pltpu.VMEM((2, NZ, RH, NX), f32),
            pltpu.VMEM((2, 2, NZ, HALO, NX), f32),
            pltpu.VMEM((NZ, R, NX), f32),
            pltpu.VMEM((U, planes, R, NX), f32),
            pltpu.VMEM((planes, R, NX), f32),
            pltpu.VMEM((NZ, RH, NX), f32),
            pltpu.VMEM((U, 2, C, NX), f32),
            pltpu.VMEM((T, C, NX), f32),
            dma((T,)),
            dma((T,)),
            dma((U, q, 3)),
            dma((NZ, 3)),
            dma((S,)),
            dma((S,)),
            dma((2,)),
            dma((2,)),
            dma((2,)),
            dma((2,)),
            dma((U,)),
            dma((U,)),
            dma((U, 3)),
            dma((U, 3)),
            dma((NZ,)),
            dma((U, q)),
            dma((T,)),
            dma((T,)),
        ],
        compiler_params=pltpu.CompilerParams(
            has_side_effects=True, vmem_limit_bytes=48 * 1024 * 1024
        ),
    )(forcing.reshape(zl * NY, NX), stacked)
    return out.reshape(forcing.shape)


def solution(mesh):
    return jax.shard_map(
        body,
        mesh=mesh,
        in_specs=(
            P("tm", "space", None, None),
            P("space", None, None),
            P("space", None, None),
            P(None, "space", None, None),
        ),
        out_specs=P("tm", "space", None, None),
        check_vma=False,
    )
```

```python
import math

import jax
import jax.numpy as jnp
import numpy as np
from jax import lax
from jax.experimental import pallas as pl
from jax.experimental.pallas import tpu as pltpu
from jax.sharding import PartitionSpec as P

ITERS = 2
SWEEPS = 8
HALO = 8

wrap_alpha = 0.1


def forward_table(steps):
    n = np.arange(steps)
    gamma = wrap_alpha ** (n / steps)
    table = np.zeros((steps // 2, 2, steps))
    for u in range(steps // 2):
        angle = 2.0 * np.pi * ((u * n) % steps) / steps
        if u == 0:
            table[u, 0] = gamma
            table[u, 1] = (1.0 - 2.0 * (n % 2)) * gamma
        else:
            table[u, 0] = np.cos(angle) * gamma
            table[u, 1] = -np.sin(angle) * gamma
    return table


def inverse_table(steps):
    n = np.arange(steps)
    table = np.zeros((steps // 2, 2, steps))
    for u in range(steps // 2):
        angle = 2.0 * np.pi * ((u * n) % steps) / steps
        if u == 0:
            table[u, 0] = 1.0 / steps
            table[u, 1] = (1.0 - 2.0 * (n % 2)) / steps
        else:
            table[u, 0] = 2.0 * np.cos(angle) / steps
            table[u, 1] = -2.0 * np.sin(angle) / steps
    return table


def by_index(index, values):
    picked = jnp.float32(values[0])
    for at in range(1, len(values)):
        picked = jnp.where(index == at, jnp.float32(values[at]), picked)
    return picked


def kernel(
    dims,
    f_ref,
    k_ref,
    out_ref,
    times,
    fields,
    edge,
    kbuf,
    coef,
    pq,
    src,
    wa,
    wb,
    whalo,
    part,
    gathered,
    reduced,
    last,
    back,
    states,
    s1,
    r1,
    s2,
    r2,
    sk,
    rk,
    se,
    re,
    sw,
    rw,
    ss,
    rs,
    sg,
    rg,
    s3,
    r3,
    s4,
    r4,
):
    T, S, NY, NX, zl = dims
    U = T // 2
    NZ = zl * S
    C = zl * NY // T
    bands = 2 * S
    R = NY // bands
    RH = R + 2 * HALO
    q = C // R
    planes = NZ // U
    rho = wrap_alpha ** (1.0 / T)
    forward = forward_table(T)
    inverse = inverse_table(T)
    n = np.arange(T)
    gamma = wrap_alpha ** (n / T)

    t = lax.axis_index("tm")
    s = lax.axis_index("space")
    group = t // zl
    zi = t % zl
    unit = (zi * S + s) // q
    band = group * q + (zi * S + s) % q
    row0 = pl.multiple_of(group * C, 8)

    def place(u, b):
        at = u * q + b % q
        return (b // q) * zl + at // S, at % S

    def chunk(tt):
        start = (tt % zl) * NY + (tt // zl) * C
        return pl.ds(pl.multiple_of(start, 8), C)

    far_first = sorted(range(1, T), key=lambda d: -min(d, T - d))

    def device(tt, ts):
        return {"tm": tt, "space": ts}

    def remote(source, target, ssem, rsem, tt, ts):
        return pltpu.make_async_remote_copy(
            src_ref=source,
            dst_ref=target,
            send_sem=ssem,
            recv_sem=rsem,
            device_id=device(tt, ts),
            device_id_type=pl.DeviceIdType.MESH,
        )

    barrier = pltpu.get_barrier_semaphore()
    for d in range(1, T):
        pl.semaphore_signal(barrier, inc=1, device_id=device(lax.rem(t + d, T), s), device_id_type=pl.DeviceIdType.MESH)
    for d in range(1, S):
        pl.semaphore_signal(barrier, inc=1, device_id=device(t, lax.rem(s + d, S)), device_id_type=pl.DeviceIdType.MESH)
    pl.semaphore_wait(barrier, T + S - 2)
    sent = []

    def send(source, target, ssem, rsem, tt, ts, valid=None, maybe_self=True):
        copy = remote(source, target, ssem, rsem, tt, ts)
        same = jnp.logical_and(tt == t, ts == s) if maybe_self else None
        away = valid
        if maybe_self:
            here = same if valid is None else jnp.logical_and(valid, same)
            away = jnp.logical_not(same)
            if valid is not None:
                away = jnp.logical_and(valid, away)

            @pl.when(here)
            def _():
                pltpu.make_async_copy(source, target, rsem).start()

        if away is None:
            copy.start()
            sent.append(copy.wait_send)
        else:

            @pl.when(away)
            def _():
                copy.start()

            def finish():
                @pl.when(away)
                def _():
                    copy.wait_send()

            sent.append(finish)

    def arrived(target, rsem, valid=None):
        if valid is None:
            pltpu.make_async_copy(target, target, rsem).wait()
        else:

            @pl.when(valid)
            def _():
                pltpu.make_async_copy(target, target, rsem).wait()

    for d in far_first:
        tt = lax.rem(t + d, T)
        send(
            f_ref.at[chunk(tt)],
            times.at[t],
            s1.at[d],
            r1.at[d],
            tt,
            s,
            maybe_self=False,
        )
    send(
        k_ref.at[4, zl - 1, pl.ds(row0 + HALO, C)],
        edge.at[0],
        se.at[0],
        re.at[0],
        t,
        jnp.minimum(s + 1, S - 1),
        valid=s + 1 < S,
        maybe_self=False,
    )
    send(
        k_ref.at[4, 0, pl.ds(row0 + HALO, C)],
        edge.at[1],
        se.at[1],
        re.at[1],
        t,
        jnp.maximum(s - 1, 0),
        valid=s > 0,
        maybe_self=False,
    )
    for d in range(1, S):
        ts = lax.rem(s + d, S)
        rows = pl.ds(pl.multiple_of((group * q + (zi * S + ts) % q) * R, 8), RH)
        source = k_ref.at[pl.ds(0, 4), :, rows]
        target = kbuf.at[:, pl.ds(s * zl, zl)]
        send(source, target, sk.at[d], rk.at[d], t, ts, maybe_self=False)
    times[pl.ds(t, 1)] = f_ref[chunk(t)][None]

    angles = [2.0 * math.pi * u / U / 2 for u in range(U)]
    shift_re1 = by_index(unit, [rho * math.cos(a) for a in angles])
    shift_im1 = by_index(unit, [0.0] + [rho * math.sin(a) for a in angles[1:]])
    shift_re2 = by_index(unit, [-rho] + [rho * math.cos(a) for a in angles[1:]])
    wide_column = lax.broadcasted_iota(jnp.int32, (RH, NX), 1)

    def prepare(z, c, vz, vy, vx):
        az = c * vz
        ay = c * vy
        ax = c * vx
        zero = jnp.zeros_like(c)
        coef[0, z] = jnp.where(z == NZ - 1, zero, c - az)
        coef[1, z] = jnp.where(z == 0, zero, c + az)
        coef[2, z] = c - ay
        coef[3, z] = c + ay
        coef[4, z] = jnp.where(wide_column == NX - 1, zero, c - ax)
        coef[5, z] = jnp.where(wide_column == 0, zero, c + ax)
        diag1 = 1.0 + 6.0 * c - shift_re1
        diag2 = 1.0 + 6.0 * c - shift_re2
        im2 = shift_im1 * shift_im1
        modulus1 = diag1 * diag1 + im2
        modulus2 = diag2 * diag2 + im2
        pq[0, z] = diag1 / modulus1
        pq[1, z] = diag2 / modulus2
        pq[2, z] = shift_im1 / modulus1

    band_rows = pl.ds(pl.multiple_of(band * R, 8), RH)
    for o in range(zl):
        prepare(s * zl + o, *[k_ref[m, o, band_rows] for m in range(4)])

    def shifted(value, by, axis):
        return pltpu.roll(value, by % value.shape[axis], axis)

    window = pl.ds(row0, C + 2 * HALO)
    inner = pl.ds(row0 + HALO, C)
    column = lax.broadcasted_iota(jnp.int32, (C, NX), 1)
    arrived(edge.at[0], re.at[0], valid=s > 0)
    arrived(edge.at[1], re.at[1], valid=s + 1 < S)

    @pl.when(s == 0)
    def _():
        edge[0] = jnp.zeros((C, NX), jnp.float32)

    @pl.when(s + 1 == S)
    def _():
        edge[1] = jnp.zeros((C, NX), jnp.float32)

    wide = k_ref[4, zi, window]
    middle = wide[HALO : HALO + C]
    lower = jnp.where(zi == 0, edge[0], k_ref[4, jnp.maximum(zi - 1, 0), inner])
    upper = jnp.where(zi == zl - 1, edge[1], k_ref[4, jnp.minimum(zi + 1, zl - 1), inner])
    coupling = k_ref[0, zi, inner]
    adz = coupling * k_ref[1, zi, inner]
    ady = coupling * k_ref[2, zi, inner]
    adx = coupling * k_ref[3, zi, inner]
    summed = (coupling - adz) * upper + (coupling + adz) * lower
    summed += (coupling - ady) * shifted(wide, -1, 0)[HALO : HALO + C]
    summed += (coupling + ady) * shifted(wide, 1, 0)[HALO : HALO + C]
    summed += (coupling - adx) * jnp.where(column == NX - 1, 0.0, shifted(middle, -1, 1))
    summed += (coupling + adx) * jnp.where(column == 0, 0.0, shifted(middle, 1, 1))
    start = summed - 6.0 * coupling * middle

    for d in range(1, T):
        arrived(times.at[lax.rem(t + T - d, T)], r1.at[d])

    for block in range(C // 8):
        rows = slice(block * 8, block * 8 + 8)
        values = [times[m, rows] + start[rows] for m in range(T)]
        for u in range(U):
            for p in range(2):
                total = values[0] * float(forward[u, p, 0])
                for m in range(1, T):
                    total = total + values[m] * float(forward[u, p, m])
                fields[u, p, rows] = total

    z = s * zl + zi
    for step in range(U):
        u = lax.rem(unit + step, U)
        for o in range(q):
            b = group * q + o
            for kind in range(3):
                to = b + (0, -1, 1)[kind]
                valid = (None, to >= 0, to < bands)[kind]
                safe = jnp.clip(to, 0, bands - 1)
                first, count, land = (
                    (o * R, R, HALO),
                    (o * R, HALO, HALO + R),
                    (o * R + R - HALO, HALO, 0),
                )[kind]
                to_t, to_s = place(u, safe)
                send(
                    fields.at[u, :, pl.ds(first, count)],
                    src.at[:, z, pl.ds(land, count)],
                    s2.at[step, o, kind],
                    r2.at[z, kind],
                    to_t,
                    to_s,
                    valid=valid,
                )

    for d in range(1, S):
        theirs = lax.rem(s + S - d, S) * zl
        arrived(kbuf.at[:, pl.ds(theirs, zl)], rk.at[d])
        for o in range(zl):
            prepare(theirs + o, *[kbuf[m, theirs + o] for m in range(4)])

    @pl.when(band == 0)
    def _():
        src[:, :, :HALO] = jnp.zeros((2, NZ, HALO, NX), jnp.float32)
        last[:, :HALO] = jnp.zeros((NZ, HALO, NX), jnp.float32)
        whalo[0] = jnp.zeros((2, NZ, HALO, NX), jnp.float32)

    @pl.when(band == bands - 1)
    def _():
        src[:, :, HALO + R :] = jnp.zeros((2, NZ, HALO, NX), jnp.float32)
        last[:, HALO + R :] = jnp.zeros((NZ, HALO, NX), jnp.float32)
        whalo[1] = jnp.zeros((2, NZ, HALO, NX), jnp.float32)

    for z in range(NZ):
        arrived(src.at[:, z, pl.ds(HALO, R)], r2.at[z, 0])
        arrived(src.at[:, z, pl.ds(HALO + R, HALO)], r2.at[z, 1], valid=band < bands - 1)
        arrived(src.at[:, z, pl.ds(0, HALO)], r2.at[z, 2], valid=band > 0)

    def scale(z, re_part, im_part, target):
        p1, p2, im = pq[0, z], pq[1, z], pq[2, z]
        target[0, z] = re_part * p1 + im_part * im
        target[1, z] = im_part * p2 - re_part * im

    together = math.gcd(NZ, 8)

    def sweep(old, new):
        @pl.loop(0, NZ // together)
        def _(trip):
            for o in range(together):
                z = trip * together + o
                up = jnp.minimum(z + 1, NZ - 1) if o == together - 1 else z + 1
                down = jnp.maximum(z - 1, 0) if o == 0 else z - 1
                sums = []
                for p in range(2):
                    here = old[p, z]
                    total = src[p, z] + coef[0, z] * old[p, up] + coef[1, z] * old[p, down]
                    total += coef[2, z] * shifted(here, -1, 0) + coef[3, z] * shifted(here, 1, 0)
                    total += coef[4, z] * shifted(here, -1, 1) + coef[5, z] * shifted(here, 1, 1)
                    sums.append(total)
                scale(z, sums[0], sums[1], new)

    @pl.loop(0, NZ)
    def _(z):
        scale(z, src[0, z], src[1, z], wa)

    @pl.loop(0, SWEEPS // 2)
    def _(i):
        sweep(wa, wb)
        sweep(wb, wa)

    below = jnp.maximum(band - 1, 0)
    above = jnp.minimum(band + 1, bands - 1)
    send(
        wa.at[:, :, pl.ds(HALO + R - HALO, HALO)],
        whalo.at[0],
        sw.at[0],
        rw.at[0],
        *place(unit, above),
        valid=band < bands - 1,
        maybe_self=False,
    )
    send(
        wa.at[:, :, pl.ds(HALO, HALO)],
        whalo.at[1],
        sw.at[1],
        rw.at[1],
        *place(unit, below),
        valid=band > 0,
        maybe_self=False,
    )
    weight_re = by_index(unit, [float(inverse[u, 0, T - 1]) for u in range(U)])
    weight_im = by_index(unit, [float(inverse[u, 1, T - 1]) for u in range(U)])

    @pl.loop(0, NZ)
    def _(z):
        part[z] = weight_re * wa[0, z, HALO : HALO + R] + weight_im * wa[1, z, HALO : HALO + R]

    for d in range(1, U):
        u = lax.rem(unit + d, U)
        send(
            part.at[pl.ds(u * planes, planes)],
            gathered.at[unit],
            ss.at[d],
            rs.at[d],
            *place(u, band),
            maybe_self=False,
        )
    gathered[pl.ds(unit, 1)] = part[pl.ds(unit * planes, planes)][None]
    for d in range(1, U):
        arrived(gathered.at[lax.rem(unit + U - d, U)], rs.at[d])
    total = gathered[0]
    for u in range(1, U):
        total = total + gathered[u]
    reduced[...] = total * rho
    mine = pl.ds(unit * planes, planes)
    for d in range(U):
        u = lax.rem(unit + d, U)
        for kind in range(3):
            to = band + (0, -1, 1)[kind]
            valid = (None, to >= 0, to < bands)[kind]
            safe = jnp.clip(to, 0, bands - 1)
            first, count, land = ((0, R, HALO), (0, HALO, HALO + R), (R - HALO, HALO, 0))[kind]
            if kind == 0 and d == 0:
                last[mine, HALO : HALO + R] = reduced[...]
                continue
            send(
                reduced.at[:, pl.ds(first, count)],
                last.at[mine, pl.ds(land, count)],
                sg.at[d, kind],
                rg.at[d, kind],
                *place(u, safe),
                valid=valid,
                maybe_self=False,
            )
    arrived(whalo.at[0], rw.at[0], valid=band > 0)
    arrived(whalo.at[1], rw.at[1], valid=band < bands - 1)
    sent_before = list(sent)
    sent.clear()
    for finish in sent_before:
        finish()
    wa[:, :, :HALO] = whalo[0]
    wa[:, :, HALO + R :] = whalo[1]
    for d in range(U):
        theirs = pl.ds(lax.rem(unit + U - d, U) * planes, planes)
        if d:
            arrived(last.at[theirs, pl.ds(HALO, R)], rg.at[d, 0])
        arrived(last.at[theirs, pl.ds(HALO + R, HALO)], rg.at[d, 1], valid=band < bands - 1)
        arrived(last.at[theirs, pl.ds(0, HALO)], rg.at[d, 2], valid=band > 0)

    @pl.loop(0, NZ)
    def _(z):
        src[0, z] = src[0, z] - last[z]
        src[1, z] = src[1, z] - jnp.where(unit == 0, last[z], jnp.zeros_like(last[z]))

    @pl.loop(0, SWEEPS // 2)
    def _(i):
        sweep(wa, wb)
        sweep(wb, wa)

    sweep(wa, wb)

    for step in range(NZ):
        z = lax.rem(unit * planes + step, NZ)
        at = group * zl + z % zl
        offset = pl.multiple_of((band % q) * R, 8)
        send(
            wb.at[:, z, pl.ds(HALO, R)],
            back.at[unit, :, pl.ds(offset, R)],
            s3.at[step],
            r3.at[unit, lax.rem(band, q)],
            at,
            z // zl,
        )
    for u in range(U):
        for o in range(q):
            arrived(back.at[u, :, pl.ds(o * R, R)], r3.at[u, o])
    for block in range(C // 8):
        rows = slice(block * 8, block * 8 + 8)
        values = [back[u, p, rows] for u in range(U) for p in range(2)]
        begin = middle[rows]
        for m in range(T):
            total = begin
            for at in range(T):
                total = total + values[at] * float(inverse[at // 2, at % 2, m] / gamma[m])
            states[m, rows] = total
    for d in far_first:
        tt = lax.rem(t + d, T)
        send(
            states.at[tt],
            out_ref.at[chunk(t)],
            s4.at[d],
            r4.at[d],
            tt,
            s,
            maybe_self=False,
        )
    out_ref[chunk(t)] = states[pl.ds(t, 1)][0]
    for d in range(1, T):
        tt = lax.rem(t + T - d, T)
        arrived(out_ref.at[chunk(tt)], r4.at[d])
    for finish in sent:
        finish()


def body(forcing, initial, coupling, velocity):
    local_steps, zl, NY, NX = forcing.shape
    T = lax.axis_size("tm")
    S = lax.axis_size("space")
    U = T // 2
    NZ = zl * S
    C = zl * NY // T
    bands = 2 * S
    R = NY // bands
    RH = R + 2 * HALO
    q = C // R
    planes = NZ // U
    assert local_steps == 1 and SWEEPS <= HALO <= R and ITERS == 2
    assert C % R == 0 and NY % C == 0 and NZ % U == 0
    stacked = jnp.concatenate([coupling[None], velocity, initial[None]], axis=0)
    stacked = jnp.pad(stacked, ((0, 0), (0, 0), (HALO, HALO), (0, 0)))
    f32 = jnp.float32
    dma = pltpu.SemaphoreType.DMA
    out = pl.pallas_call(
        lambda *refs: kernel((T, S, NY, NX, zl), *refs),
        out_shape=jax.ShapeDtypeStruct((zl * NY, NX), f32),
        in_specs=[pl.BlockSpec(memory_space=pltpu.VMEM)] * 2,
        out_specs=pl.BlockSpec(memory_space=pltpu.VMEM),
        scratch_shapes=[
            pltpu.VMEM((T, C, NX), f32),
            pltpu.VMEM((U, 2, C, NX), f32),
            pltpu.VMEM((2, C, NX), f32),
            pltpu.VMEM((4, NZ, RH, NX), f32),
            pltpu.VMEM((6, NZ, RH, NX), f32),
            pltpu.VMEM((3, NZ, RH, NX), f32),
            pltpu.VMEM((2, NZ, RH, NX), f32),
            pltpu.VMEM((2, NZ, RH, NX), f32),
            pltpu.VMEM((2, NZ, RH, NX), f32),
            pltpu.VMEM((2, 2, NZ, HALO, NX), f32),
            pltpu.VMEM((NZ, R, NX), f32),
            pltpu.VMEM((U, planes, R, NX), f32),
            pltpu.VMEM((planes, R, NX), f32),
            pltpu.VMEM((NZ, RH, NX), f32),
            pltpu.VMEM((U, 2, C, NX), f32),
            pltpu.VMEM((T, C, NX), f32),
            dma((T,)),
            dma((T,)),
            dma((U, q, 3)),
            dma((NZ, 3)),
            dma((S,)),
            dma((S,)),
            dma((2,)),
            dma((2,)),
            dma((2,)),
            dma((2,)),
            dma((U,)),
            dma((U,)),
            dma((U, 3)),
            dma((U, 3)),
            dma((NZ,)),
            dma((U, q)),
            dma((T,)),
            dma((T,)),
        ],
        compiler_params=pltpu.CompilerParams(
            has_side_effects=True, collective_id=0, vmem_limit_bytes=48 * 1024 * 1024
        ),
    )(forcing.reshape(zl * NY, NX), stacked)
    return out.reshape(forcing.shape)


def solution(mesh):
    return jax.shard_map(
        body,
        mesh=mesh,
        in_specs=(
            P("tm", "space", None, None),
            P("space", None, None),
            P("space", None, None),
            P(None, "space", None, None),
        ),
        out_specs=P("tm", "space", None, None),
        check_vma=False,
    )
```

```python
import math

import jax
import jax.numpy as jnp
import numpy as np
from jax import lax
from jax.experimental import pallas as pl
from jax.experimental.pallas import tpu as pltpu
from jax.sharding import PartitionSpec as P

ITERS = 2
SWEEPS = 8
HALO = 8

wrap_alpha = 0.1


def forward_table(steps):
    n = np.arange(steps)
    gamma = wrap_alpha ** (n / steps)
    table = np.zeros((steps // 2, 2, steps))
    for u in range(steps // 2):
        angle = 2.0 * np.pi * ((u * n) % steps) / steps
        if u == 0:
            table[u, 0] = gamma
            table[u, 1] = (1.0 - 2.0 * (n % 2)) * gamma
        else:
            table[u, 0] = np.cos(angle) * gamma
            table[u, 1] = -np.sin(angle) * gamma
    return table


def inverse_table(steps):
    n = np.arange(steps)
    table = np.zeros((steps // 2, 2, steps))
    for u in range(steps // 2):
        angle = 2.0 * np.pi * ((u * n) % steps) / steps
        if u == 0:
            table[u, 0] = 1.0 / steps
            table[u, 1] = (1.0 - 2.0 * (n % 2)) / steps
        else:
            table[u, 0] = 2.0 * np.cos(angle) / steps
            table[u, 1] = -2.0 * np.sin(angle) / steps
    return table


def by_index(index, values):
    picked = jnp.float32(values[0])
    for at in range(1, len(values)):
        picked = jnp.where(index == at, jnp.float32(values[at]), picked)
    return picked


def kernel(
    dims,
    f_ref,
    k_ref,
    out_ref,
    times,
    fields,
    edge,
    kbuf,
    coef,
    pq,
    src,
    wa,
    wb,
    whalo,
    part,
    gathered,
    reduced,
    last,
    back,
    states,
    s1,
    r1,
    s2,
    r2,
    sk,
    rk,
    sf,
    rf,
    se,
    re,
    sw,
    rw,
    ss,
    rs,
    sg,
    rg,
    s3,
    r3,
    s4,
    r4,
):
    T, S, NY, NX, zl = dims
    U = T // 2
    NZ = zl * S
    C = zl * NY // T
    bands = 2 * S
    R = NY // bands
    RH = R + 2 * HALO
    q = C // R
    planes = NZ // U
    rho = wrap_alpha ** (1.0 / T)
    forward = forward_table(T)
    inverse = inverse_table(T)
    n = np.arange(T)
    gamma = wrap_alpha ** (n / T)

    t = lax.axis_index("tm")
    s = lax.axis_index("space")
    group = t // zl
    zi = t % zl
    unit = (zi * S + s) // q
    band = group * q + (zi * S + s) % q
    row0 = pl.multiple_of(group * C, 8)

    def place(u, b):
        at = u * q + b % q
        return (b // q) * zl + at // S, at % S

    def chunk(tt):
        start = (tt % zl) * NY + (tt // zl) * C
        return pl.ds(pl.multiple_of(start, 8), C)

    ring = range(1, T)

    def device(tt, ts):
        return {"tm": tt, "space": ts}

    def remote(source, target, ssem, rsem, tt, ts):
        return pltpu.make_async_remote_copy(
            src_ref=source,
            dst_ref=target,
            send_sem=ssem,
            recv_sem=rsem,
            device_id=device(tt, ts),
            device_id_type=pl.DeviceIdType.MESH,
        )

    barrier = pltpu.get_barrier_semaphore()
    for d in range(1, T):
        pl.semaphore_signal(barrier, inc=1, device_id=device(lax.rem(t + d, T), s), device_id_type=pl.DeviceIdType.MESH)
    for d in range(1, S):
        pl.semaphore_signal(barrier, inc=1, device_id=device(t, lax.rem(s + d, S)), device_id_type=pl.DeviceIdType.MESH)
    pl.semaphore_wait(barrier, T + S - 2)
    sent = []

    def send(source, target, ssem, rsem, tt, ts, valid=None, maybe_self=True):
        copy = remote(source, target, ssem, rsem, tt, ts)
        same = jnp.logical_and(tt == t, ts == s) if maybe_self else None
        away = valid
        if maybe_self:
            here = same if valid is None else jnp.logical_and(valid, same)
            away = jnp.logical_not(same)
            if valid is not None:
                away = jnp.logical_and(valid, away)

            @pl.when(here)
            def _():
                pltpu.make_async_copy(source, target, rsem).start()

        if away is None:
            copy.start()
            sent.append(copy.wait_send)
        else:

            @pl.when(away)
            def _():
                copy.start()

            def finish():
                @pl.when(away)
                def _():
                    copy.wait_send()

            sent.append(finish)

    def arrived(target, rsem, valid=None):
        if valid is None:
            pltpu.make_async_copy(target, target, rsem).wait()
        else:

            @pl.when(valid)
            def _():
                pltpu.make_async_copy(target, target, rsem).wait()

    for d in ring:
        tt = lax.rem(t + d, T)
        send(
            f_ref.at[chunk(tt)],
            times.at[t],
            s1.at[d],
            r1.at[d],
            tt,
            s,
            maybe_self=False,
        )
    send(
        k_ref.at[4, zl - 1, pl.ds(row0 + HALO, C)],
        edge.at[0],
        se.at[0],
        re.at[0],
        t,
        jnp.minimum(s + 1, S - 1),
        valid=s + 1 < S,
        maybe_self=False,
    )
    send(
        k_ref.at[4, 0, pl.ds(row0 + HALO, C)],
        edge.at[1],
        se.at[1],
        re.at[1],
        t,
        jnp.maximum(s - 1, 0),
        valid=s > 0,
        maybe_self=False,
    )
    half = zl // 2
    share = (t % 2) * half
    rest = half - share
    partner = t + 1 - 2 * (t % 2)
    for d in range(1, S):
        ts = lax.rem(s + d, S)
        rows = pl.ds(pl.multiple_of((group * q + (zi * S + ts) % q) * R, 8), RH)
        source = k_ref.at[pl.ds(0, 4), pl.ds(share, half), rows]
        target = kbuf.at[:, pl.ds(s * zl + share, half)]
        send(source, target, sk.at[d], rk.at[d], t, ts, maybe_self=False)
    times[pl.ds(t, 1)] = f_ref[chunk(t)][None]

    angles = [2.0 * math.pi * u / U / 2 for u in range(U)]
    shift_re1 = by_index(unit, [rho * math.cos(a) for a in angles])
    shift_im1 = by_index(unit, [0.0] + [rho * math.sin(a) for a in angles[1:]])
    shift_re2 = by_index(unit, [-rho] + [rho * math.cos(a) for a in angles[1:]])
    wide_column = lax.broadcasted_iota(jnp.int32, (RH, NX), 1)

    def prepare(z, c, vz, vy, vx):
        az = c * vz
        ay = c * vy
        ax = c * vx
        zero = jnp.zeros_like(c)
        coef[0, z] = jnp.where(z == NZ - 1, zero, c - az)
        coef[1, z] = jnp.where(z == 0, zero, c + az)
        coef[2, z] = c - ay
        coef[3, z] = c + ay
        coef[4, z] = jnp.where(wide_column == NX - 1, zero, c - ax)
        coef[5, z] = jnp.where(wide_column == 0, zero, c + ax)
        diag1 = 1.0 + 6.0 * c - shift_re1
        diag2 = 1.0 + 6.0 * c - shift_re2
        im2 = shift_im1 * shift_im1
        modulus1 = diag1 * diag1 + im2
        modulus2 = diag2 * diag2 + im2
        pq[0, z] = diag1 / modulus1
        pq[1, z] = diag2 / modulus2
        pq[2, z] = shift_im1 / modulus1

    band_rows = pl.ds(pl.multiple_of(band * R, 8), RH)
    for o in range(zl):
        prepare(s * zl + o, *[k_ref[m, o, band_rows] for m in range(4)])

    def shifted(value, by, axis):
        return pltpu.roll(value, by % value.shape[axis], axis)

    window = pl.ds(row0, C + 2 * HALO)
    inner = pl.ds(row0 + HALO, C)
    column = lax.broadcasted_iota(jnp.int32, (C, NX), 1)
    arrived(edge.at[0], re.at[0], valid=s > 0)
    arrived(edge.at[1], re.at[1], valid=s + 1 < S)

    @pl.when(s == 0)
    def _():
        edge[0] = jnp.zeros((C, NX), jnp.float32)

    @pl.when(s + 1 == S)
    def _():
        edge[1] = jnp.zeros((C, NX), jnp.float32)

    wide = k_ref[4, zi, window]
    middle = wide[HALO : HALO + C]
    lower = jnp.where(zi == 0, edge[0], k_ref[4, jnp.maximum(zi - 1, 0), inner])
    upper = jnp.where(zi == zl - 1, edge[1], k_ref[4, jnp.minimum(zi + 1, zl - 1), inner])
    coupling = k_ref[0, zi, inner]
    adz = coupling * k_ref[1, zi, inner]
    ady = coupling * k_ref[2, zi, inner]
    adx = coupling * k_ref[3, zi, inner]
    summed = (coupling - adz) * upper + (coupling + adz) * lower
    summed += (coupling - ady) * shifted(wide, -1, 0)[HALO : HALO + C]
    summed += (coupling + ady) * shifted(wide, 1, 0)[HALO : HALO + C]
    summed += (coupling - adx) * jnp.where(column == NX - 1, 0.0, shifted(middle, -1, 1))
    summed += (coupling + adx) * jnp.where(column == 0, 0.0, shifted(middle, 1, 1))
    start = summed - 6.0 * coupling * middle

    for d in range(1, T):
        arrived(times.at[lax.rem(t + T - d, T)], r1.at[d])

    for block in range(C // 8):
        rows = slice(block * 8, block * 8 + 8)
        values = [times[m, rows] + start[rows] for m in range(T)]
        for u in range(U):
            for p in range(2):
                total = values[0] * float(forward[u, p, 0])
                for m in range(1, T):
                    total = total + values[m] * float(forward[u, p, m])
                fields[u, p, rows] = total

    z = s * zl + zi
    for step in range(U):
        u = lax.rem(unit + step, U)
        for o in range(q):
            b = group * q + o
            for kind in range(3):
                to = b + (0, -1, 1)[kind]
                valid = (None, to >= 0, to < bands)[kind]
                safe = jnp.clip(to, 0, bands - 1)
                first, count, land = (
                    (o * R, R, HALO),
                    (o * R, HALO, HALO + R),
                    (o * R + R - HALO, HALO, 0),
                )[kind]
                to_t, to_s = place(u, safe)
                send(
                    fields.at[u, :, pl.ds(first, count)],
                    src.at[:, z, pl.ds(land, count)],
                    s2.at[step, o, kind],
                    r2.at[z, kind],
                    to_t,
                    to_s,
                    valid=valid,
                )

    for d in range(1, S):
        theirs = lax.rem(s + S - d, S) * zl
        block = kbuf.at[:, pl.ds(theirs + share, half)]
        arrived(block, rk.at[d])
        send(block, block, sf.at[d], rf.at[d], partner, s, maybe_self=False)
    for d in range(1, S):
        theirs = lax.rem(s + S - d, S) * zl
        for o in range(half):
            at = theirs + share + o
            prepare(at, *[kbuf[m, at] for m in range(4)])
        arrived(kbuf.at[:, pl.ds(theirs + rest, half)], rf.at[d])
        for o in range(half):
            at = theirs + rest + o
            prepare(at, *[kbuf[m, at] for m in range(4)])

    @pl.when(band == 0)
    def _():
        src[:, :, :HALO] = jnp.zeros((2, NZ, HALO, NX), jnp.float32)
        last[:, :HALO] = jnp.zeros((NZ, HALO, NX), jnp.float32)
        whalo[0] = jnp.zeros((2, NZ, HALO, NX), jnp.float32)

    @pl.when(band == bands - 1)
    def _():
        src[:, :, HALO + R :] = jnp.zeros((2, NZ, HALO, NX), jnp.float32)
        last[:, HALO + R :] = jnp.zeros((NZ, HALO, NX), jnp.float32)
        whalo[1] = jnp.zeros((2, NZ, HALO, NX), jnp.float32)

    for z in range(NZ):
        arrived(src.at[:, z, pl.ds(HALO, R)], r2.at[z, 0])
        arrived(src.at[:, z, pl.ds(HALO + R, HALO)], r2.at[z, 1], valid=band < bands - 1)
        arrived(src.at[:, z, pl.ds(0, HALO)], r2.at[z, 2], valid=band > 0)

    def scale(z, re_part, im_part, target):
        p1, p2, im = pq[0, z], pq[1, z], pq[2, z]
        target[0, z] = re_part * p1 + im_part * im
        target[1, z] = im_part * p2 - re_part * im

    together = math.gcd(NZ, 8)

    def sweep(old, new):
        @pl.loop(0, NZ // together)
        def _(trip):
            for o in range(together):
                z = trip * together + o
                up = jnp.minimum(z + 1, NZ - 1) if o == together - 1 else z + 1
                down = jnp.maximum(z - 1, 0) if o == 0 else z - 1
                sums = []
                for p in range(2):
                    here = old[p, z]
                    total = src[p, z] + coef[0, z] * old[p, up] + coef[1, z] * old[p, down]
                    total += coef[2, z] * shifted(here, -1, 0) + coef[3, z] * shifted(here, 1, 0)
                    total += coef[4, z] * shifted(here, -1, 1) + coef[5, z] * shifted(here, 1, 1)
                    sums.append(total)
                scale(z, sums[0], sums[1], new)

    @pl.loop(0, NZ)
    def _(z):
        scale(z, src[0, z], src[1, z], wa)

    @pl.loop(0, SWEEPS // 2)
    def _(i):
        sweep(wa, wb)
        sweep(wb, wa)

    below = jnp.maximum(band - 1, 0)
    above = jnp.minimum(band + 1, bands - 1)
    send(
        wa.at[:, :, pl.ds(HALO + R - HALO, HALO)],
        whalo.at[0],
        sw.at[0],
        rw.at[0],
        *place(unit, above),
        valid=band < bands - 1,
        maybe_self=False,
    )
    send(
        wa.at[:, :, pl.ds(HALO, HALO)],
        whalo.at[1],
        sw.at[1],
        rw.at[1],
        *place(unit, below),
        valid=band > 0,
        maybe_self=False,
    )
    weight_re = by_index(unit, [float(inverse[u, 0, T - 1]) for u in range(U)])
    weight_im = by_index(unit, [float(inverse[u, 1, T - 1]) for u in range(U)])

    @pl.loop(0, NZ)
    def _(z):
        part[z] = weight_re * wa[0, z, HALO : HALO + R] + weight_im * wa[1, z, HALO : HALO + R]

    for d in range(1, U):
        u = lax.rem(unit + d, U)
        send(
            part.at[pl.ds(u * planes, planes)],
            gathered.at[unit],
            ss.at[d],
            rs.at[d],
            *place(u, band),
            maybe_self=False,
        )
    gathered[pl.ds(unit, 1)] = part[pl.ds(unit * planes, planes)][None]
    for d in range(1, U):
        arrived(gathered.at[lax.rem(unit + U - d, U)], rs.at[d])
    total = gathered[0]
    for u in range(1, U):
        total = total + gathered[u]
    reduced[...] = total * rho
    mine = pl.ds(unit * planes, planes)
    for d in range(U):
        u = lax.rem(unit + d, U)
        for kind in range(3):
            to = band + (0, -1, 1)[kind]
            valid = (None, to >= 0, to < bands)[kind]
            safe = jnp.clip(to, 0, bands - 1)
            first, count, land = ((0, R, HALO), (0, HALO, HALO + R), (R - HALO, HALO, 0))[kind]
            if kind == 0 and d == 0:
                last[mine, HALO : HALO + R] = reduced[...]
                continue
            send(
                reduced.at[:, pl.ds(first, count)],
                last.at[mine, pl.ds(land, count)],
                sg.at[d, kind],
                rg.at[d, kind],
                *place(u, safe),
                valid=valid,
                maybe_self=False,
            )
    arrived(whalo.at[0], rw.at[0], valid=band > 0)
    arrived(whalo.at[1], rw.at[1], valid=band < bands - 1)
    sent_before = list(sent)
    sent.clear()
    for finish in sent_before:
        finish()
    wa[:, :, :HALO] = whalo[0]
    wa[:, :, HALO + R :] = whalo[1]
    for d in range(U):
        theirs = pl.ds(lax.rem(unit + U - d, U) * planes, planes)
        if d:
            arrived(last.at[theirs, pl.ds(HALO, R)], rg.at[d, 0])
        arrived(last.at[theirs, pl.ds(HALO + R, HALO)], rg.at[d, 1], valid=band < bands - 1)
        arrived(last.at[theirs, pl.ds(0, HALO)], rg.at[d, 2], valid=band > 0)

    @pl.loop(0, NZ)
    def _(z):
        src[0, z] = src[0, z] - last[z]
        src[1, z] = src[1, z] - jnp.where(unit == 0, last[z], jnp.zeros_like(last[z]))

    @pl.loop(0, SWEEPS // 2)
    def _(i):
        sweep(wa, wb)
        sweep(wb, wa)

    sweep(wa, wb)

    for step in range(NZ):
        z = lax.rem(unit * planes + step, NZ)
        at = group * zl + z % zl
        offset = pl.multiple_of((band % q) * R, 8)
        send(
            wb.at[:, z, pl.ds(HALO, R)],
            back.at[unit, :, pl.ds(offset, R)],
            s3.at[step],
            r3.at[unit, lax.rem(band, q)],
            at,
            z // zl,
        )
    for u in range(U):
        for o in range(q):
            arrived(back.at[u, :, pl.ds(o * R, R)], r3.at[u, o])
    for block in range(C // 8):
        rows = slice(block * 8, block * 8 + 8)
        values = [back[u, p, rows] for u in range(U) for p in range(2)]
        begin = middle[rows]
        for m in range(T):
            total = begin
            for at in range(T):
                total = total + values[at] * float(inverse[at // 2, at % 2, m] / gamma[m])
            states[m, rows] = total
    for d in ring:
        tt = lax.rem(t + d, T)
        send(
            states.at[tt],
            out_ref.at[chunk(t)],
            s4.at[d],
            r4.at[d],
            tt,
            s,
            maybe_self=False,
        )
    out_ref[chunk(t)] = states[pl.ds(t, 1)][0]
    for d in range(1, T):
        tt = lax.rem(t + T - d, T)
        arrived(out_ref.at[chunk(tt)], r4.at[d])
    for finish in sent:
        finish()


def body(forcing, initial, coupling, velocity):
    local_steps, zl, NY, NX = forcing.shape
    T = lax.axis_size("tm")
    S = lax.axis_size("space")
    U = T // 2
    NZ = zl * S
    C = zl * NY // T
    bands = 2 * S
    R = NY // bands
    RH = R + 2 * HALO
    q = C // R
    planes = NZ // U
    assert local_steps == 1 and SWEEPS <= HALO <= R and ITERS == 2
    assert S % q == 0 and zl % 2 == 0 and T % 2 == 0
    assert C % R == 0 and NY % C == 0 and NZ % U == 0
    stacked = jnp.concatenate([coupling[None], velocity, initial[None]], axis=0)
    stacked = jnp.pad(stacked, ((0, 0), (0, 0), (HALO, HALO), (0, 0)))
    f32 = jnp.float32
    dma = pltpu.SemaphoreType.DMA
    out = pl.pallas_call(
        lambda *refs: kernel((T, S, NY, NX, zl), *refs),
        out_shape=jax.ShapeDtypeStruct((zl * NY, NX), f32),
        in_specs=[pl.BlockSpec(memory_space=pltpu.VMEM)] * 2,
        out_specs=pl.BlockSpec(memory_space=pltpu.VMEM),
        scratch_shapes=[
            pltpu.VMEM((T, C, NX), f32),
            pltpu.VMEM((U, 2, C, NX), f32),
            pltpu.VMEM((2, C, NX), f32),
            pltpu.VMEM((4, NZ, RH, NX), f32),
            pltpu.VMEM((6, NZ, RH, NX), f32),
            pltpu.VMEM((3, NZ, RH, NX), f32),
            pltpu.VMEM((2, NZ, RH, NX), f32),
            pltpu.VMEM((2, NZ, RH, NX), f32),
            pltpu.VMEM((2, NZ, RH, NX), f32),
            pltpu.VMEM((2, 2, NZ, HALO, NX), f32),
            pltpu.VMEM((NZ, R, NX), f32),
            pltpu.VMEM((U, planes, R, NX), f32),
            pltpu.VMEM((planes, R, NX), f32),
            pltpu.VMEM((NZ, RH, NX), f32),
            pltpu.VMEM((U, 2, C, NX), f32),
            pltpu.VMEM((T, C, NX), f32),
            dma((T,)),
            dma((T,)),
            dma((U, q, 3)),
            dma((NZ, 3)),
            dma((S,)),
            dma((S,)),
            dma((S,)),
            dma((S,)),
            dma((2,)),
            dma((2,)),
            dma((2,)),
            dma((2,)),
            dma((U,)),
            dma((U,)),
            dma((U, 3)),
            dma((U, 3)),
            dma((NZ,)),
            dma((U, q)),
            dma((T,)),
            dma((T,)),
        ],
        compiler_params=pltpu.CompilerParams(
            has_side_effects=True, collective_id=0, vmem_limit_bytes=48 * 1024 * 1024
        ),
    )(forcing.reshape(zl * NY, NX), stacked)
    return out.reshape(forcing.shape)


def solution(mesh):
    return jax.shard_map(
        body,
        mesh=mesh,
        in_specs=(
            P("tm", "space", None, None),
            P("space", None, None),
            P("space", None, None),
            P(None, "space", None, None),
        ),
        out_specs=P("tm", "space", None, None),
        check_vma=False,
    )
```
